256 devices in a mesh: tp: 4 (over x), dp: 64 (over z, y, core).
Axes of the slice: x: 4, y: 4, z: 8, core: 2. Of those that a mesh axis runs over, the one named last changes fastest.
Arguments:
- item_query: bfloat16 [8192, 2048], P('dp', 'tp'), may hold values from -20 to 20, as said below
- item_keys: bfloat16 [8192, 4, 2048], P('dp', None, 'tp'), may hold values from -20 to 20
- item_values: bfloat16 [8192, 4, 2048], P('dp', None, 'tp'), may hold values from -6 to 6
- item_out_weight: bfloat16 [2048, 4096], P('tp'), may hold values from -0.125 to 0.125
- item_residual: bfloat16 [8192, 4096], P('dp'), may hold values from -3 to 3
- cite_home: int32 [65536, 1], P('dp'), may hold values from 0 to 63; in each aligned block of 1024 rows (0 to 1023, 1024 to 2047, ...) at most 24 rows name the same one
- cite_row: int32 [65536], P('dp'), may hold values from 0 to 127
- seq_length: int32 [64], P('dp'), may hold values from 1 to 1024, 40960 in all
- user_gain: float32 [4096], replicated, may hold values from 0.1 to 1.9
- user_weight: bfloat16 [4096, 16, 384], P('dp', 'tp'), may hold values from -0.09375 to 0.09375
Outputs:
- user_qkv: bfloat16 [65536, 16, 384], P('dp', 'tp')
The draws below stay inside these ranges and needn't reach their ends.
Inputs may be any that keep to these rules, and one draw needn't show every extreme that they name: `item_query`: in hidden draws some items' queries equal a multiple of keys at their last two tokens. `cite_home`: among the 1024 positions of one sequence at most 24 cite items of one home device, and some home device is cited exactly 24 times. `seq_length`: some sequence has all 1024 positions live.
All inputs are finite; a program needn't handle non-finite values. No bound on the sum of `seq_length` on one device may be relied on, other than what follows from the above.
Results may differ from the reference program's by a relative error of at most 0.0065.
Values may be sent and summed in bfloat16 or wider, within the bound.
No kernel may reach another device: no remote copies, remote signals or barrier semaphores. Data moves between devices by JAX's collectives and lax.ppermute only.
A program may use at most 128 MiB of HBM per device.

```python
import math
import jax
import jax.numpy as jnp
import numpy as np
from jax import lax

D = 4096
HEADS = 16
HEAD_DIM = 128
ITEMS_DEV = 128
ITEM_TOK = 4
USER_LEN = 1024
CAP = 24
ITEMS = 8192
ROWS = 65536
N_DP = 64


def paired_draw(key):
    base = jax.random.fold_in(key, 911)
    key_query, key_keys = jax.random.split(base, 2)
    queries = jnp.clip(jax.random.normal(key_query, (ITEMS, HEADS, HEAD_DIM), jnp.float32), -4.0, 4.0)
    keys_all = jnp.clip(jax.random.normal(key_keys, (ITEMS, ITEM_TOK, HEADS, HEAD_DIM), jnp.float32), -4.0, 4.0)
    return (queries, keys_all)


def draw_item_query(key, part):
    queries, keys_all = paired_draw(key)
    return queries.reshape(ITEMS, HEADS * HEAD_DIM).astype(jnp.bfloat16)


def draw_item_keys(key, part):
    queries, keys_all = paired_draw(key)
    return keys_all.reshape(ITEMS, ITEM_TOK, HEADS * HEAD_DIM).astype(jnp.bfloat16)


def set_ends(entries, own_key, smallest, high):
    spot = [jax.random.randint(jax.random.fold_in(own_key, axis), (), 0, length) for axis, length in enumerate(entries.shape)]
    longest = entries.shape.index(max(entries.shape))
    neighbour = spot[:longest] + [(spot[longest] + 1) % entries.shape[longest]] + spot[longest + 1:]
    return entries.at[tuple(spot)].set(smallest).at[tuple(neighbour)].set(high)


def steps_of(own_key, dims, shards, least, top_value):
    level, own = 1.0, jax.random.fold_in(own_key, 6)
    for axis_at, shards_of in shards:
        heights = jnp.exp(jax.random.uniform(jax.random.fold_in(own, axis_at), (shards_of,), jnp.float32, least / len(shards), top_value / len(shards)))
        level = level * jnp.repeat(heights, dims[axis_at] // shards_of).reshape([-1 if axis == axis_at else 1 for axis in range(len(dims))])
    return level


def length_profile(amount, total, reach, lean):
    portions = [(1 << 20) // math.isqrt(standing ** lean) + 1 for standing in range(2, amount + 1)]
    spare, given = total - reach - (amount - 1), [1] * (amount - 1)
    while spare > 0:
        free = [i for i in range(amount - 1) if given[i] < reach]
        mass, left = sum([portions[i] for i in free]), spare
        for i in free:
            more = min(reach - given[i], max(1, left * portions[i] // mass), spare)
            given[i] = given[i] + more
            spare = spare - more
    return np.array([reach] + given)


def ragged_sizes(rng, count, total, limit, skew):
    if count == 2:
        one = jax.random.randint(rng, (), max(1, total - limit), min(limit, total - 1) + 1)
        return jnp.stack([one, total - one])
    sizes = jnp.asarray(length_profile(count, total, limit, skew), jnp.int32)
    twos = (count - 1) // 2
    giver, receiver = sizes[1:1 + 2 * twos:2], sizes[2:2 + 2 * twos:2]
    room = jnp.minimum(giver - 1, limit - receiver)
    moved = jax.random.randint(jax.random.fold_in(rng, 1), (twos,), 0, 1 << 20) % (room + 1)
    sizes = sizes.at[1:1 + 2 * twos:2].set(giver - moved).at[2:2 + 2 * twos:2].set(receiver + moved)
    return sizes[jax.random.permutation(jax.random.fold_in(rng, 2), count)]


def deal_out(key, own, number, rows, count, top, most, skew):
    ranking = jax.random.permutation(key, count)
    heavy_load, ordinary = shares(count, rows * top, most, skew, True), shares(count, rows * top, most, skew, False)
    places = jnp.arange(count)

    def named(sizes, offset_by):
        used = int((sizes > 0).sum())
        fixed = max(1, used // 4)
        moved = fixed + (places - fixed + offset_by * (used - fixed)) % max(1, count - fixed)
        return jnp.zeros((count,), jnp.int32).at[ranking[jnp.where(places < fixed, places, moved)]].set(jnp.asarray(sizes, jnp.int32))

    sizes = jnp.where(number % 4 == 0, named(heavy_load, number // 4), named(ordinary, number - number // 4 - 1))
    mixed = jax.random.permutation(jax.random.fold_in(own, 3), count)
    source_of, taker = mixed[0:count // 2 * 2:2], mixed[1:count // 2 * 2:2]
    slack = jnp.minimum(sizes[source_of] - 1, most - sizes[taker]) // 2
    slack = jnp.where((source_of == ranking[0]) | (taker == ranking[0]) | (sizes[taker] == 0), 0, jnp.maximum(slack, 0))
    moved = jax.random.randint(jax.random.fold_in(own, 4), (count // 2,), 0, 1 << 20) % (slack + 1)
    sizes = sizes.at[source_of].add(-moved).at[taker].add(moved)
    members = jnp.searchsorted(jnp.cumsum(sizes), jnp.arange(rows * top), side="right").astype(jnp.int32)
    listing = members.reshape(top, rows).T
    listing = listing[jax.random.permutation(jax.random.fold_in(own, 1), rows)]
    offset_by = jax.random.randint(jax.random.fold_in(own, 2), (rows, 1), 0, top)
    return jnp.take_along_axis(listing, (jnp.arange(top)[None, :] + offset_by) % top, axis=1)


def shares(amount, total, limit, slope, full):
    loads = [(1 << 20) // math.isqrt(rank ** slope) + 1 for rank in range(1, amount + 1)]
    largest = limit if full else min(limit, max(-(-total // amount), total * loads[0] // sum(loads)))
    least = 1 if total - largest >= amount - 1 else 0
    given, spare = [largest] + [least] * (amount - 1), total - largest - least * (amount - 1)
    while spare > 0:
        free = [i for i in range(1, amount) if given[i] < largest] or [i for i in range(1, amount) if given[i] < limit]
        mass, remaining = sum([loads[i] for i in free]), spare
        for i in free:
            extra = min(limit - given[i], max(1, remaining * loads[i] // mass), spare)
            given[i] = given[i] + extra
            spare = spare - extra
    return np.array(given)


def normal_values(key, shape, spread, reach, cuts=(), held_as=jnp.bfloat16):
    values = spread * jax.random.normal(key, shape, jnp.float32)
    if cuts:
        values = values * steps_of(key, shape, cuts, -0.22, 0.18)
    return jnp.clip(values, -reach, reach).astype(held_as)


def setup_inputs(seed: int = 0) -> dict:
    streams_of = jax.random.split(jax.random.key(seed), 11)
    item_query = draw_item_query(jax.random.fold_in(streams_of[10], 71), 0)
    item_keys = draw_item_keys(jax.random.fold_in(streams_of[10], 71), 0)
    item_values = normal_values(streams_of[2], (ITEMS, ITEM_TOK, HEADS * HEAD_DIM), 1.0, 6.0, ((0, 64), (2, 4)))
    item_out_weight = normal_values(streams_of[3], (HEADS * HEAD_DIM, D), (HEADS * HEAD_DIM) ** -0.5, 0.125, ((0, 4),))
    item_residual = normal_values(streams_of[4], (ITEMS, D), 0.5, 3.0, ((0, 64),))
    cite_home_keys = jax.random.split(jax.random.fold_in(streams_of[5], 1), ROWS // USER_LEN)
    cite_home_turns = jax.random.permutation(jax.random.fold_in(streams_of[5], 3), ROWS // USER_LEN)
    cite_home = jax.vmap(lambda own, number: deal_out(jax.random.fold_in(streams_of[5], 2), own, number, USER_LEN, N_DP, 1, CAP, 2))(cite_home_keys, cite_home_turns).reshape((ROWS, 1))
    cite_row = set_ends(jax.random.randint(streams_of[6], (ROWS,), 0, ITEMS_DEV), jax.random.fold_in(streams_of[6], 1), 0, ITEMS_DEV - 1).astype(jnp.int32)
    seq_length = ragged_sizes(streams_of[7], N_DP, N_DP * USER_LEN * 5 // 8, USER_LEN, 2).astype(jnp.int32)
    user_gain = jnp.clip(1.0 + 0.18 * jax.random.normal(streams_of[8], (D,), jnp.float32), 0.1, 1.9)
    user_weight = normal_values(streams_of[9], (D, HEADS, 3 * HEAD_DIM), D ** -0.5, 0.09375, ((0, 64), (1, 4)))
    return dict(item_query=item_query, item_keys=item_keys, item_values=item_values, item_out_weight=item_out_weight, item_residual=item_residual, cite_home=cite_home, cite_row=cite_row, seq_length=seq_length, user_gain=user_gain, user_weight=user_weight)


def item_block(block):
    queries, keys_all, values_all = block
    count = queries.shape[0]
    queries = queries.astype(jnp.float32).reshape(count, HEADS, HEAD_DIM)
    keys_all = keys_all.astype(jnp.float32).reshape(count, ITEM_TOK, HEADS, HEAD_DIM)
    values_all = values_all.astype(jnp.float32).reshape(count, ITEM_TOK, HEADS, HEAD_DIM)
    scores = jnp.einsum('ihd,ithd->iht', queries, keys_all, precision=lax.Precision.HIGHEST) * (1.0 / math.sqrt(HEAD_DIM))
    probs = jax.nn.softmax(scores, axis=-1).astype(jnp.bfloat16).astype(jnp.float32)
    attended = jnp.einsum('iht,ithd->ihd', probs, values_all, precision=lax.Precision.HIGHEST)
    return attended.astype(jnp.bfloat16).reshape(count, HEADS * HEAD_DIM)

def reference(item_query, item_keys, item_values, item_out_weight, item_residual, cite_home, cite_row, seq_length, user_gain, user_weight):
    blocks = (item_query.reshape(N_DP, ITEMS_DEV, HEADS * HEAD_DIM), item_keys.reshape(N_DP, ITEMS_DEV, ITEM_TOK, HEADS * HEAD_DIM), item_values.reshape(N_DP, ITEMS_DEV, ITEM_TOK, HEADS * HEAD_DIM))
    attended = lax.map(item_block, blocks).reshape(N_DP * ITEMS_DEV, HEADS * HEAD_DIM)
    mixed = jnp.dot(attended, item_out_weight, preferred_element_type=jnp.float32)
    item_vec = (mixed + item_residual.astype(jnp.float32)).astype(jnp.bfloat16)
    index = (cite_home[:, 0] * ITEMS_DEV + cite_row).astype(jnp.int32)
    cited = jnp.take(item_vec, index, axis=0).reshape(N_DP, USER_LEN, D)
    weight_flat = user_weight.reshape(D, HEADS * 3 * HEAD_DIM)

    def owner(pair):
        rows, length = pair
        values32 = rows.astype(jnp.float32)
        scale = lax.rsqrt(lax.optimization_barrier(jnp.mean(values32 * values32, axis=1, keepdims=True)) + 1e-05)
        normed = (values32 * scale * user_gain[None, :]).astype(jnp.bfloat16)
        projected = jnp.dot(normed, weight_flat, preferred_element_type=jnp.float32)
        live = jnp.arange(USER_LEN, dtype=jnp.int32) < length
        return jnp.where(live[:, None], projected, jnp.zeros_like(projected)).astype(jnp.bfloat16)
    result = lax.map(owner, (cited, seq_length))
    return result.reshape(N_DP * USER_LEN, HEADS, 3 * HEAD_DIM)
```

```python
import math

import jax
import jax.numpy as jnp
from jax import lax
from jax.sharding import Mesh, PartitionSpec as P

HEAD_DIM = 128
CAP = 24
NX, NZ, NY, NC = 4, 8, 4, 2
BF = jnp.bfloat16
F32 = jnp.float32


DZ_ORDER = (0, 1, 7, 2, 6, 3, 5, 4)
STAGES = ((0, 3), (3, 5), (5, 7), (7, 8))


def shift(x, axis, by, size):
    return lax.ppermute(x, axis, [(i, (i + by) % size) for i in range(size)])


def ring(x, axis, size):
    blocks = [None] * size
    blocks[0] = ahead = behind = x
    for k in range(1, size // 2):
        behind = shift(behind, axis, 1, size)
        ahead = shift(ahead, axis, -1, size)
        blocks[size - k] = behind
        blocks[k] = ahead
    half = x.shape[0] // 2
    blocks[size // 2] = jnp.concatenate(
        [shift(behind[:half], axis, 1, size), shift(ahead[half:], axis, -1, size)], axis=0
    )
    return blocks


def plane_perm(dy, dc, back=False):
    sign = -1 if back else 1
    return [
        (y * NC + c, ((y + sign * dy) % NY) * NC + (c ^ dc)) for y in range(NY) for c in range(NC)
    ]


def onehot(a, b):
    return (a == b).astype(BF)


def dot(a, b):
    return jnp.dot(a, b, preferred_element_type=F32)


def item_attention(item_query, item_keys, item_values):
    items, width = item_query.shape
    tokens = item_keys.shape[1]
    heads = width // HEAD_DIM
    queries = item_query.reshape(items, heads, HEAD_DIM)
    keys = item_keys.reshape(items, tokens, heads, HEAD_DIM)
    values = item_values.reshape(items, tokens, heads, HEAD_DIM)
    scores = jnp.einsum("ihd,ithd->iht", queries, keys, preferred_element_type=F32) * (
        1.0 / math.sqrt(HEAD_DIM)
    )
    probs = jax.nn.softmax(scores, axis=-1).astype(BF)
    attended = jnp.einsum("iht,ithd->ihd", probs, values, preferred_element_type=F32)
    return attended.astype(BF).reshape(items, width)


def per_device(
    item_query, item_keys, item_values, item_out_weight, item_residual,
    cite_home, cite_row, seq_length, user_gain, user_weight,
):
    x, z, y, c = (lax.axis_index(n) for n in ("tp", "z", "y", "core"))
    items = item_query.shape[0]
    width = item_out_weight.shape[1]
    length = cite_home.shape[0]
    rows, heads, triple = user_weight.shape
    cols = heads * triple

    weight = user_weight.reshape(rows, cols)
    half = rows // 2
    by_z = jnp.concatenate(ring(weight[:half], "z", NZ), axis=0)
    path_zy = ring(by_z, "y", NY)
    by_y = jnp.concatenate(ring(weight[half:], "y", NY), axis=0)
    path_yz = ring(by_y, "z", NZ)

    quarter = width // NX
    attended = item_attention(item_query, item_keys, item_values)
    partial = dot(attended, item_out_weight)

    def piece(a, s):
        return lax.dynamic_slice_in_dim(a, ((x + s) % NX) * quarter, quarter, 1)

    summed = piece(partial, 0)
    for s in (1, 2, 3):
        summed = summed + shift(piece(partial, s).astype(BF), "tp", s, NX).astype(F32)
    item_vec = (summed + piece(item_residual, 0).astype(F32)).astype(BF)
    vec32 = item_vec.astype(F32)
    squares = jnp.sum(vec32 * vec32, axis=1, keepdims=True)
    total = squares
    for s in (1, 2, 3):
        total = total + shift(squares, "tp", s, NX)
    scale = lax.rsqrt(total / width + 1e-05)
    gained = (vec32 * lax.dynamic_slice_in_dim(user_gain, x * quarter, quarter, 0)[None, :]).astype(BF)

    span = quarter // 2
    feat = lax.broadcasted_iota(jnp.int32, (quarter, span), 0)
    at = lax.broadcasted_iota(jnp.int32, (quarter, span), 1)
    pick = (at // rows) * (2 * rows) + at % rows
    mine = dot(gained, onehot(feat, pick + c * rows)).astype(BF)
    theirs = dot(gained, onehot(feat, pick + (1 - c) * rows)).astype(BF)
    both = jnp.concatenate([mine, shift(theirs, "core", 1, NC)], axis=0)
    spread = jnp.concatenate([both] + [shift(both, "tp", s, NX) for s in (1, 2, 3)], axis=1)

    depth = NX * span
    src = lax.broadcasted_iota(jnp.int32, (depth, depth), 0)
    pos = lax.broadcasted_iota(jnp.int32, (1, depth), 1)
    zy_first = pos < depth // 2
    q = pos % (depth // 2)
    dy = jnp.where(zy_first, q // (NZ * half), (q // half) % NY)
    dz = jnp.where(zy_first, (q // half) % NZ, q // (NY * half))
    row = q % half + jnp.where(zy_first, 0, half)
    zy = ((z + dz) % NZ) * NY + (y + dy) % NY
    per_x = NZ * NY // NX
    where = ((x - zy // per_x) % NX) * span + (zy % per_x) * rows + row
    lined = dot(spread, onehot(src, where)).astype(BF)

    product = None
    start = 0
    for block in path_zy + path_yz:
        n = block.shape[0]
        term = dot(lined[:, start : start + n], block)
        product = term if product is None else product + term
        start += n
    projected = product[:items] + shift(product[items:], "core", 1, NC)
    item_qkv = (projected * scale).astype(BF)

    home = cite_home
    order = jnp.zeros_like(home)
    delta = ((home // (NY * NC)) - z) % NZ
    for i, d in enumerate(DZ_ORDER):
        order = jnp.where(delta == d, i, order)
    peer = ((((home // NC) % NY) - y) % NY) * NC + ((home % NC) ^ c)
    key = peer * NZ + order
    keys = NY * NC * NZ
    marks = onehot(key, lax.broadcasted_iota(jnp.int32, (1, keys), 1))
    r0 = lax.broadcasted_iota(jnp.int32, (length, length), 0)
    r1 = lax.broadcasted_iota(jnp.int32, (length, length), 1)
    before = dot((r1 < r0).astype(BF), marks)
    slot = jnp.sum(before * marks.astype(F32), axis=1, keepdims=True).astype(jnp.int32)
    live = lax.broadcasted_iota(jnp.int32, (length, 1), 0) < seq_length[0]
    target = jnp.where(live, key * CAP + slot, -1)
    slots = keys * CAP
    placed = onehot(target, lax.broadcasted_iota(jnp.int32, (1, slots), 1))
    wanted = lax.dot_general(
        cite_row.astype(BF)[None, :], placed, (((1,), (0,)), ((), ())), preferred_element_type=F32
    ).astype(jnp.int32)
    per_peer = NZ * CAP
    peers = [(dy_, dc_) for dy_ in range(NY) for dc_ in range(NC)]
    asked = []
    for p, (dy_, dc_) in enumerate(peers):
        ask = wanted[:, p * per_peer : (p + 1) * per_peer]
        if p:
            ask = lax.ppermute(ask, ("y", "core"), plane_perm(dy_, dc_))
        asked.append(ask)

    column = ring(item_qkv, "z", NZ)
    result = None
    for lo, hi in STAGES:
        n = (hi - lo) * CAP
        rows_asked = jnp.concatenate([a[:, lo * CAP : hi * CAP] for a in asked], axis=1).reshape(-1, 1)
        chosen = None
        for i in range(lo, hi):
            at_i = lax.broadcasted_iota(jnp.int32, (1, n), 1) // CAP == (i - lo)
            at_i = jnp.tile(at_i, (1, len(peers))).reshape(-1, 1)
            sel = onehot(
                jnp.where(at_i, rows_asked, -1), lax.broadcasted_iota(jnp.int32, (1, items), 1)
            )
            term = dot(sel, column[DZ_ORDER[i]])
            chosen = term if chosen is None else chosen + term
        chosen = chosen.astype(BF)
        got = []
        for p, (dy_, dc_) in enumerate(peers):
            part = chosen[p * n : (p + 1) * n]
            if p:
                part = lax.ppermute(part, ("y", "core"), plane_perm(dy_, dc_, back=True))
            got.append(part)
        got = jnp.concatenate(got, axis=0)
        j = lax.broadcasted_iota(jnp.int32, (1, n * len(peers)), 1)
        j = (j // n) * per_peer + lo * CAP + j % n
        term = dot(onehot(target, j), got)
        result = term if result is None else result + term
    return result.astype(BF).reshape(length, heads, triple)


def solution(mesh):
    dp = ("z", "y", "core")
    fine = Mesh(mesh.devices.reshape(NX, NZ, NY, NC), ("tp",) + dp)
    in_specs = (
        P(dp, "tp"), P(dp, None, "tp"), P(dp, None, "tp"), P("tp", None), P(dp, None),
        P(dp, None), P(dp), P(dp), P(), P(dp, "tp", None),
    )
    return jax.shard_map(
        per_device, mesh=fine, in_specs=in_specs, out_specs=P(dp, "tp", None), check_vma=False
    )
```

```python
import math

import jax
import jax.numpy as jnp
from jax import lax
from jax.experimental import pallas as pl
from jax.experimental.pallas import tpu as pltpu
from jax.sharding import Mesh, PartitionSpec as P


HEAD_DIM = 128
CAP = 24
NX, NZ, NY, NC = 4, 8, 4, 2
BF = jnp.bfloat16
F32 = jnp.float32


DZ_ORDER = (0, 1, 7, 2, 6, 3, 5, 4)
STAGES = ((0, 3), (3, 7), (7, 8))


def shift(x, axis, by):
    size = {"tp": NX, "z": NZ, "y": NY, "core": NC}[axis]
    return lax.ppermute(x, axis, [(i, (i + by) % size) for i in range(size)])


def ring_z(x):
    blocks = [None] * NZ
    blocks[0] = ahead = behind = x
    for k in range(1, NZ // 2):
        behind = shift(behind, "z", 1)
        ahead = shift(ahead, "z", -1)
        blocks[NZ - k], blocks[k] = behind, ahead
    blocks[NZ // 2] = shift(behind, "z", 1)
    return blocks


def onehot(a, b):
    return (a == b).astype(BF)


def dot(a, b):
    return jnp.dot(a, b, preferred_element_type=F32)


def in_smem():
    return pl.BlockSpec(memory_space=pltpu.SMEM)


def in_vmem():
    return pl.BlockSpec(memory_space=pltpu.VMEM)


def serve(asked, blocks, lo):
    m = len(blocks)
    peers = asked.shape[0]
    tail = blocks[0].shape[1:]

    def body(asked_ref, *refs):
        block_refs, out_refs = refs[:m], refs[m:]
        for i in range(m):

            def one(k, carry, i=i):
                for p in range(peers):
                    out_refs[p][i * CAP + k] = block_refs[i][asked_ref[p, (lo + i) * CAP + k]]
                return carry

            lax.fori_loop(0, CAP, one, 0, unroll=2)

    return pl.pallas_call(
        body,
        in_specs=[in_smem()] + [in_vmem()] * m,
        out_specs=[in_vmem()] * peers,
        out_shape=[jax.ShapeDtypeStruct((m * CAP,) + tail, BF)] * peers,
        name="serve",
    )(asked, *blocks)


def place(spots, parts, length):
    peers = spots.shape[0]
    tail = parts[0].shape[1:]
    spare = 8

    def body(spots_ref, *refs):
        part_refs, out_ref, buffer, done = refs[:-3], refs[-3], refs[-2], refs[-1]

        def clear(k, carry):
            buffer[pl.ds(k * 8, 8)] = jnp.zeros((8,) + tail, BF)
            return carry

        lax.fori_loop(0, (length + spare) // 8, clear, 0, unroll=4)
        for k, (lo, hi) in enumerate(STAGES):

            def one(i, carry, k=k, lo=lo):
                for p in range(peers):
                    buffer[spots_ref[p, lo * CAP + i]] = part_refs[k * peers + p][i]
                return carry

            lax.fori_loop(0, (hi - lo) * CAP, one, 0, unroll=2)
        copy = pltpu.make_async_copy(buffer.at[pl.ds(0, length)], out_ref, done)
        copy.start()
        copy.wait()

    return pl.pallas_call(
        body,
        in_specs=[in_smem()] + [in_vmem()] * len(parts),
        out_specs=pl.BlockSpec(memory_space=pl.ANY),
        out_shape=jax.ShapeDtypeStruct((length,) + tail, BF),
        scratch_shapes=[pltpu.VMEM((length + spare,) + tail, BF), pltpu.SemaphoreType.DMA],
        name="place",
    )(spots, *parts)


def item_attention(item_query, item_keys, item_values):
    items, width = item_query.shape
    tokens = item_keys.shape[1]
    heads = width // HEAD_DIM
    queries = item_query.reshape(items, heads, HEAD_DIM)
    keys = item_keys.reshape(items, tokens, heads, HEAD_DIM)
    values = item_values.reshape(items, tokens, heads, HEAD_DIM)
    scores = jnp.einsum("ihd,ithd->iht", queries, keys, preferred_element_type=F32) * (
        1.0 / math.sqrt(HEAD_DIM)
    )
    probs = jax.nn.softmax(scores, axis=-1).astype(BF)
    attended = jnp.einsum("iht,ithd->ihd", probs, values, preferred_element_type=F32)
    return attended.astype(BF).reshape(items, width)


def routes(cite_home, cite_row, length_live, z, y, c):
    length = cite_home.shape[0]
    delta = ((cite_home // (NY * NC)) - z) % NZ
    order = jnp.zeros_like(cite_home)
    for i, d in enumerate(DZ_ORDER):
        order = jnp.where(delta == d, i, order)
    chip = ((cite_home // NC) % NY - y) % NY
    other = (cite_home % NC) ^ c
    key = (other * NY + chip) * NZ + order
    keys = NC * NY * NZ
    marks = onehot(key, lax.broadcasted_iota(jnp.int32, (1, keys), 1))
    r0 = lax.broadcasted_iota(jnp.int32, (length, length), 0)
    r1 = lax.broadcasted_iota(jnp.int32, (length, length), 1)
    before = dot((r1 < r0).astype(BF), marks)
    slot = jnp.sum(before * marks.astype(F32), axis=1, keepdims=True).astype(jnp.int32)
    live = lax.broadcasted_iota(jnp.int32, (length, 1), 0) < length_live
    full = jnp.where(live, key * CAP + slot, -1)
    placed = onehot(full, lax.broadcasted_iota(jnp.int32, (1, keys * CAP), 1))
    place_no = lax.broadcasted_iota(jnp.int32, (1, length), 1)
    base = 1 << 6
    facts = jnp.concatenate(
        [cite_row[None, :], place_no // base, place_no % base, jnp.ones_like(place_no)], axis=0
    )
    table = lax.dot_general(
        facts.astype(BF), placed, (((1,), (0,)), ((), ())), preferred_element_type=F32
    ).astype(jnp.int32)
    spots = jnp.where(table[3] > 0, table[1] * base + table[2], length)
    shape = (NC, NY, NZ * CAP)
    return table[0].reshape(shape), spots.reshape(NC * NY, NZ * CAP)


def per_device(
    item_query, item_keys, item_values, item_out_weight, item_residual,
    cite_home, cite_row, seq_length, user_gain, user_weight,
):
    x, z, y, c = (lax.axis_index(n) for n in ("tp", "z", "y", "core"))
    items = item_query.shape[0]
    width = item_out_weight.shape[1]
    rows, heads, triple = user_weight.shape
    cols = heads * triple

    weight = lax.all_gather(user_weight.reshape(rows, cols), ("z", "core"), axis=0, tiled=True)

    quarter = width // NX
    attended = item_attention(item_query, item_keys, item_values)
    partial = dot(attended, item_out_weight)

    def piece(a, s):
        return lax.dynamic_slice_in_dim(a, ((x + s) % NX) * quarter, quarter, 1)

    summed = piece(partial, 0)
    for s in (1, 2, 3):
        summed = summed + shift(piece(partial, s).astype(BF), "tp", s).astype(F32)
    item_vec = (summed + piece(item_residual, 0).astype(F32)).astype(BF)

    zs = NZ // NX
    unit = quarter // (zs * NY)

    def features(d):
        at = ((y + d) % NY) * unit
        parts = [
            lax.dynamic_slice_in_dim(item_vec, at + i * NY * unit, unit, 1) for i in range(zs)
        ]
        return jnp.concatenate(parts, axis=1)

    slab = [features(0)] + [shift(features(d), "y", d) for d in range(1, NY)]
    slab = jnp.concatenate(slab, axis=0)
    span = zs * unit
    spread = jnp.zeros((NY * items, NX * span), BF)
    for s in range(NX):
        block = slab if s == 0 else shift(slab, "tp", s)
        spread = lax.dynamic_update_slice_in_dim(spread, block, ((x - s) % NX) * span, 1)
    gain = lax.dynamic_slice_in_dim(user_gain.reshape(NZ, NY, unit), y, 1, 1).reshape(1, NX * span)
    vec32 = spread.astype(F32)
    gained = (vec32 * gain).astype(BF)
    squares = jnp.sum(vec32 * vec32, axis=1, keepdims=True)

    home, row_of, live_to = lax.optimization_barrier((cite_home, cite_row, seq_length, item_vec))[:3]
    wanted, spots = routes(home, row_of, live_to[0], z, y, c)
    joined = jnp.stack([wanted[0], shift(wanted[1], "core", 1)], axis=1)
    asked = [joined[0]] + [shift(joined[d], "y", d) for d in range(1, NY)]
    asked = jnp.concatenate(asked, axis=0)

    lane = lax.broadcasted_iota(jnp.int32, (items, 128), 1)
    summed = None
    for d in (2, 1, 3, 0):
        term = dot(gained[d * items : (d + 1) * items], weight)
        square = squares[d * items : (d + 1) * items]
        if d:
            high = square.astype(BF)
            rest = square - high.astype(F32)
            mid = rest.astype(BF)
            low = (rest - mid.astype(F32)).astype(BF)
            tail = jnp.where(lane == 0, high, jnp.where(lane == 1, mid, jnp.where(lane == 2, low, 0)))
            back = shift(jnp.concatenate([term.astype(BF), tail.astype(BF)], axis=1), "y", -d)
            term = back[:, :cols].astype(F32)
            square = jnp.sum(back[:, cols:].astype(F32), axis=1, keepdims=True)
        summed = (term, square) if summed is None else (summed[0] + term, summed[1] + square)
    scale = lax.rsqrt(summed[1] / width + 1e-05)
    item_qkv = (summed[0] * scale).astype(BF).reshape(items, heads, triple)

    column = ring_z(item_qkv)
    parts = []
    for lo, hi in STAGES:
        chosen = serve(asked, [column[DZ_ORDER[i]] for i in range(lo, hi)], lo)
        near, far = [], []
        for d in range(NY):
            for other, into in ((0, near), (1, far)):
                part = chosen[d * NC + other]
                if d or other:
                    pairs = [
                        (a * NC + b, ((a - d) % NY) * NC + (b ^ other))
                        for a in range(NY) for b in range(NC)
                    ]
                    part = lax.ppermute(part, ("y", "core"), pairs)
                into.append(part)
        parts += near + far
    return place(spots, parts, cite_home.shape[0])


def solution(mesh):
    dp = ("z", "y", "core")
    fine = Mesh(mesh.devices.reshape(NX, NZ, NY, NC), ("tp",) + dp)
    in_specs = (
        P(dp, "tp"), P(dp, None, "tp"), P(dp, None, "tp"), P("tp", None), P(dp, None),
        P(dp, None), P(dp), P(dp), P(), P(dp, "tp", None),
    )

    return jax.shard_map(
        per_device, mesh=fine, in_specs=in_specs, out_specs=P(dp, "tp", None), check_vma=False
    )
```
